1024 devices in a mesh: dp: 8 (over y), expert: 8 (over x), group: 16 (over z, core).
Axes of the slice: x: 8, y: 8, z: 8, core: 2. Of those that a mesh axis runs over, the one named last changes fastest.
Arguments:
- tokens: bfloat16 [2048, 7168], P(('dp', 'group')), may hold values from -6 to 6
- expert_ids: int32 [2048, 8], P(('dp', 'group')), may hold values from 0 to 255, all different within a row; in each aligned block of 16 rows (0 to 15, 16 to 31, ...) at most 2 rows name the same one
- gate_values: bfloat16 [2048, 8], P(('dp', 'group')), may hold values from 0.099609375 to 1
- gate_up: bfloat16 [8, 7168, 2, 2048], P('expert', None, None, 'group'), may hold values from -0.0625 to 0.0625
- down_weight: bfloat16 [8, 2048, 7168], P('expert', 'group'), may hold values from -0.125 to 0.125
- shared_gate_up: bfloat16 [7168, 2, 2048], P('expert', None, 'group'), may hold values from -0.0625 to 0.0625
- shared_down: bfloat16 [2048, 7168], P('group', 'expert'), may hold values from -0.125 to 0.125
Outputs:
- mixed: bfloat16 [2048, 7168], P(('dp', 'group'), 'expert')
The draws below stay inside these ranges and needn't reach their ends.
Inputs may be any that keep to these rules, and one draw needn't show every extreme that they name: `expert_ids`: each row names 8 different routed experts. In each aligned block of 16 rows (the rows of one device) no expert is named by more than 2 rows, and in some blocks one is named by exactly 2 rows.
All inputs are finite; a program needn't handle non-finite values.
Results may differ from the reference program's by a relative error of at most 0.028.
Values may be sent and summed in bfloat16 or wider, within the bound.
A program may use at most 64 MiB of HBM per device.

```python
import math
import jax
import jax.numpy as jnp
import numpy as np

D = 7168
FF = 2048
ROUTED = 256
TOPK = 8
TOK_DEV = 16
CAP = 2
SLOTS = 8
FF_DEV = 128
TOKENS = 2048
N_GROUP = 16


def block_levels(rng, dims, pieces, smallest, top_value):
    gain, own = 1.0, jax.random.fold_in(rng, 6)
    for position, parts in pieces:
        heights = jnp.exp(jax.random.uniform(jax.random.fold_in(own, position), (parts,), jnp.float32, smallest / len(pieces), top_value / len(pieces)))
        gain = gain * jnp.repeat(heights, dims[position] // parts).reshape([-1 if axis == position else 1 for axis in range(len(dims))])
    return gain


def routed_block(stream_key, own, number, rows, number_of, top, limit, skew):
    ranking = jax.random.permutation(stream_key, number_of)
    crowded, common = portions_of(number_of, rows * top, limit, skew, True), portions_of(number_of, rows * top, limit, skew, False)
    places = jnp.arange(number_of)

    def named(tallies, rotation):
        used = int((tallies > 0).sum())
        fixed = max(1, used // 4)
        moved = fixed + (places - fixed + rotation * (used - fixed)) % max(1, number_of - fixed)
        return jnp.zeros((number_of,), jnp.int32).at[ranking[jnp.where(places < fixed, places, moved)]].set(jnp.asarray(tallies, jnp.int32))

    tallies = jnp.where(number % 4 == 0, named(crowded, number // 4), named(common, number - number // 4 - 1))
    mixed = jax.random.permutation(jax.random.fold_in(own, 3), number_of)
    source_of, sink = mixed[0:number_of // 2 * 2:2], mixed[1:number_of // 2 * 2:2]
    room = jnp.minimum(tallies[source_of] - 1, limit - tallies[sink]) // 2
    room = jnp.where((source_of == ranking[0]) | (sink == ranking[0]) | (tallies[sink] == 0), 0, jnp.maximum(room, 0))
    moved = jax.random.randint(jax.random.fold_in(own, 4), (number_of // 2,), 0, 1 << 20) % (room + 1)
    tallies = tallies.at[source_of].add(-moved).at[sink].add(moved)
    members = jnp.searchsorted(jnp.cumsum(tallies), jnp.arange(rows * top), side="right").astype(jnp.int32)
    table = members.reshape(top, rows).T
    table = table[jax.random.permutation(jax.random.fold_in(own, 1), rows)]
    rotation = jax.random.randint(jax.random.fold_in(own, 2), (rows, 1), 0, top)
    return jnp.take_along_axis(table, (jnp.arange(top)[None, :] + rotation) % top, axis=1)


def portions_of(amount, total, reach, lean, full):
    weights = [(1 << 20) // math.isqrt(rank ** lean) + 1 for rank in range(1, amount + 1)]
    largest = reach if full else min(reach, max(-(-total // amount), total * weights[0] // sum(weights)))
    least = 1 if total - largest >= amount - 1 else 0
    counts, rest = [largest] + [least] * (amount - 1), total - largest - least * (amount - 1)
    while rest > 0:
        movable = [i for i in range(1, amount) if counts[i] < largest] or [i for i in range(1, amount) if counts[i] < reach]
        pool, left = sum([weights[i] for i in movable]), rest
        for i in movable:
            more = min(reach - counts[i], max(1, left * weights[i] // pool), rest)
            counts[i] = counts[i] + more
            rest = rest - more
    return np.array(counts)


def centred(key, extent, width, bound, pieces=(), dtype=jnp.bfloat16):
    result = jax.random.normal(key, extent, jnp.float32) * width
    if len(pieces) > 0:
        result = block_levels(key, extent, pieces, -0.22, 0.18) * result
    return jnp.clip(result, min=-bound, max=bound).astype(dtype)


def setup_inputs(seed: int = 0) -> dict:
    streams_of = jax.random.split(jax.random.key(seed), 8)
    tokens = centred(streams_of[0], (TOKENS, D), 1.0, 6.0, ((0, 128),))
    expert_ids_keys = jax.random.split(jax.random.fold_in(streams_of[1], 1), TOKENS // TOK_DEV)
    expert_ids_turns = jax.random.permutation(jax.random.fold_in(streams_of[1], 3), TOKENS // TOK_DEV)
    expert_ids = jax.vmap(lambda own, number: routed_block(jax.random.fold_in(streams_of[1], 2), own, number, TOK_DEV, ROUTED, TOPK, CAP, 2))(expert_ids_keys, expert_ids_turns).reshape((TOKENS, TOPK))
    gate_values = jnp.clip(jnp.exp(math.log(1.0) - 2.306499 * jax.random.uniform(streams_of[2], (TOKENS, TOPK), jnp.float32) ** block_levels(streams_of[2], (TOKENS, TOPK), ((0, 128),), -0.2, 0.2)), 0.099609375, 1.0).astype(jnp.bfloat16)
    gate_up = centred(streams_of[3], (SLOTS, D, 2, FF), D ** -0.5, 0.0625, ((0, 8), (3, 16)))
    down_weight = centred(streams_of[4], (SLOTS, FF, D), FF ** -0.5, 0.125, ((0, 8), (1, 16)))
    shared_gate_up = centred(streams_of[5], (D, 2, FF), D ** -0.5, 0.0625, ((0, 8), (2, 16)))
    shared_down = centred(streams_of[6], (FF, D), FF ** -0.5, 0.125, ((0, 16), (1, 8)))
    return {"tokens": tokens, "expert_ids": expert_ids, "gate_values": gate_values, "gate_up": gate_up, "down_weight": down_weight, "shared_gate_up": shared_gate_up, "shared_down": shared_down}


def reference(tokens, expert_ids, gate_values, gate_up, down_weight, shared_gate_up, shared_down):
    accumulated = jnp.zeros((TOKENS, D), jnp.float32)
    for slot_index in range(SLOTS):
        chosen = expert_ids == slot_index
        slot_weight = jnp.sum(jnp.where(chosen, gate_values.astype(jnp.float32), jnp.float32(0.0)), axis=1)
        gate_part = jnp.dot(tokens, gate_up[slot_index, :, 0, :], preferred_element_type=jnp.float32)
        up_part = jnp.dot(tokens, gate_up[slot_index, :, 1, :], preferred_element_type=jnp.float32)
        hidden = (jax.nn.silu(gate_part) * up_part).astype(jnp.bfloat16)
        for block_index in range(N_GROUP):
            first_unit = block_index * FF_DEV
            product = jnp.dot(hidden[:, first_unit:first_unit + FF_DEV],
                              down_weight[slot_index, first_unit:first_unit + FF_DEV, :],
                              preferred_element_type=jnp.float32)
            slot_term = (product * slot_weight[:, None]).astype(jnp.bfloat16)
            accumulated = accumulated + slot_term.astype(jnp.float32)
    shared_gate = jnp.dot(tokens, shared_gate_up[:, 0, :], preferred_element_type=jnp.float32)
    shared_up = jnp.dot(tokens, shared_gate_up[:, 1, :], preferred_element_type=jnp.float32)
    shared_hidden = (jax.nn.silu(shared_gate) * shared_up).astype(jnp.bfloat16)
    for block_index in range(N_GROUP):
        first_unit = block_index * FF_DEV
        shared_term = jnp.dot(shared_hidden[:, first_unit:first_unit + FF_DEV],
                              shared_down[first_unit:first_unit + FF_DEV, :],
                              preferred_element_type=jnp.float32).astype(jnp.bfloat16)
        accumulated = accumulated + shared_term.astype(jnp.float32)
    return accumulated.astype(jnp.bfloat16)
```

```python
import functools

import jax
import jax.numpy as jnp
from jax import lax
from jax.experimental import pallas as pl
from jax.experimental.pallas import tpu as pltpu
from jax.sharding import PartitionSpec as P

MESH = pl.DeviceIdType.MESH
CAP = 2
F32, BF16 = jnp.float32, jnp.bfloat16
GATHER_S, GATHER_R, SPREAD, SHARE, RETURN_R, RETURN_S = range(6)
SENDS, ARRIVALS = 6, 3


def iota(shape, dim):
    return lax.broadcasted_iota(jnp.int32, shape, dim)


def one_hot(condition):
    return jnp.where(condition, 1.0, 0.0).astype(BF16)


def dot(a, b):
    return jnp.dot(a, b, preferred_element_type=F32)


def swap_matrix(n):
    rows = 2 * n * n
    to, source = iota((rows, rows), 0), iota((rows, rows), 1)
    major, minor, pick = to // (2 * n), to % (2 * n) // 2, to % 2
    return one_hot(source == minor * (2 * n) + major * 2 + pick)


def kernel(
    n,
    tok_hbm,
    ids_hbm,
    val_hbm,
    w1_hbm,
    w2_hbm,
    s1_hbm,
    s2_hbm,
    out_ref,
    tok,
    ids,
    val,
    w1,
    w2,
    s1,
    s2,
    s1d,
    xs,
    xr,
    part,
    parts,
    hid,
    hids,
    spread,
    y,
    placed,
    ret_s,
    got_s,
    swap,
    expand,
    apart,
    local_sem,
    pair_send,
    pair_recv,
    send_sem,
    recv_sem,
):
    x = lax.axis_index("expert")
    g = lax.axis_index("group")
    z, c = g // 2, g % 2
    rows, width = tok.shape[1], tok.shape[2]
    units = w2.shape[1]
    pieces = width // 128
    total = n * rows

    def z_peer(k):
        return {"group": (z + k) % n * 2 + c}

    def x_peer(k):
        return {"expert": (x + k) % n}

    sibling = {"group": z * 2 + 1 - c}

    columns = pltpu.make_async_copy(
        tok_hbm.at[:, pl.ds(pl.multiple_of(x * width, 128), width)], xs.at[z], local_sem.at[6]
    )
    columns.start()
    barrier = pltpu.get_barrier_semaphore()
    peers = [z_peer(k) for k in (2, n - 2, 1, n - 1)] + [sibling]
    peers += [x_peer(k) for k in range(1, n)]
    for peer in peers:
        pl.semaphore_signal(barrier, inc=1, device_id=peer, device_id_type=MESH)

    tokens = [
        pltpu.make_async_copy(
            tok_hbm.at[:, pl.ds(j * width, width)], tok.at[j], local_sem.at[7]
        )
        for j in range(n)
    ]
    loads = [
        pltpu.make_async_copy(source, target, local_sem.at[i])
        for i, (source, target) in enumerate(
            (
                (ids_hbm, ids),
                (val_hbm, val),
                (s1_hbm, s1.at[c]),
                (s2_hbm, s2.at[c]),
                (w1_hbm, w1.at[c]),
                (w2_hbm, w2.at[c]),
            )
        )
    ]
    for copy in [*tokens, *loads]:
        copy.start()

    def send(phase, step, source, target, peer):
        pltpu.make_async_remote_copy(
            src_ref=source,
            dst_ref=target,
            send_sem=send_sem.at[phase],
            recv_sem=recv_sem.at[phase, step],
            device_id=peer,
            device_id_type=MESH,
        ).start()

    def bytes_of(ref, sem):
        pltpu.make_async_copy(ref, ref, sem).wait()

    def arrived(phase, step, target):
        bytes_of(target, recv_sem.at[phase, step])

    upper = z >= n // 2
    middle = (z >= 2) & (z < n - 2)

    far_first = sorted(range(1, n), key=lambda k: (-min(k, n - k), k))
    def at(k):
        return (z + k + n) % n

    def gather_start(phase, block, steps):
        for k in steps:
            send(phase, {2: 0, -2: 1}.get(k, 2), block.at[z], block.at[z], z_peer(k % n))

    def relay(phase, block, sign):
        source = at(-2 * sign)
        arrived(phase, 0 if sign > 0 else 1, block.at[source])
        send(phase, 2, block.at[source], block.at[source], z_peer(sign % n))

        @pl.when(middle)
        def _():
            send(phase, 2, block.at[source], block.at[source], z_peer(2 * sign % n))

    def in_turn(*steps):
        @pl.when(upper)
        def _():
            for sign in (1, -1):
                for step in steps:
                    step(sign)

        @pl.when(jnp.logical_not(upper))
        def _():
            for sign in (-1, 1):
                for step in steps:
                    step(sign)

    def gather_end(phase, block):
        arrived(phase, 2, block.at[pl.ds(0, 5)])

    def gather_sent(phase, block):
        @pl.when(middle)
        def _():
            bytes_of(block, send_sem.at[phase])

        @pl.when(jnp.logical_not(middle))
        def _():
            bytes_of(block.at[pl.ds(0, 6)], send_sem.at[phase])

    columns.wait()
    pl.semaphore_wait(barrier, len(peers))
    gather_start(GATHER_S, xs, (2, -2, 1, -1))
    pairs = [
        pltpu.make_async_remote_copy(
            src_ref=source,
            dst_ref=target.at[c],
            send_sem=pair_send.at[i],
            recv_sem=pair_recv.at[i],
            device_id=sibling,
            device_id_type=MESH,
        )
        for i, (source, target) in enumerate(
            ((s1_hbm, s1), (w1_hbm, w1), (w2_hbm, w2), (s2_hbm, s2))
        )
    ]
    pairs[0].start()

    bytes_of(tok, local_sem.at[7])
    loads[0].wait()
    named = jnp.sum(jnp.where(ids[...] == x, 1.0, 0.0), axis=0, keepdims=True)
    named = jnp.broadcast_to(named, (8, rows)).astype(BF16)
    token, lane = iota((rows, total), 0), iota((rows, total), 1)
    named_at = dot(named, one_hot(lane % rows == token))[0:1]
    place_of = dot(named, one_hot(token < lane % rows))[0:1]
    row, lane = iota((CAP * n, total), 0), iota((CAP * n, total), 1)
    picker = (named_at > 0.5) & (place_of.astype(jnp.int32) == row % CAP)
    picker = one_hot(picker & (row // CAP == lane // rows))
    packed = dot(picker, tok[...].reshape(total, width)).astype(BF16)
    xr[z] = packed
    gather_start(GATHER_R, xr, (2, -2, 1, -1))
    for copy in pairs[1:]:
        copy.start()

    def pair_arrived(i, target):
        pltpu.make_async_remote_copy(
            src_ref=target.at[1 - c],
            dst_ref=target.at[1 - c],
            send_sem=pair_send.at[i],
            recv_sem=pair_recv.at[i],
            device_id=sibling,
            device_id_type=MESH,
        ).wait_recv()

    swap[...] = swap_matrix(n)
    feature, lane = iota((128, 512), 0), iota((128, 512), 1)
    expand[...] = one_hot(lane % 256 == feature * 2 + lane // 256)
    to, source = iota((256, 256), 0), iota((256, 256), 1)
    apart[...] = one_hot(source == to % 128 * 2 + to // 128)

    loads[1].wait()
    number = iota((CAP * n, rows), 0)
    holds = jnp.zeros((CAP * n, rows), F32)
    weight = jnp.zeros((CAP * n, rows), F32)
    for k in range(ids.shape[0]):
        same = ids[k : k + 1, :] == number // CAP
        holds = holds + jnp.where(same, 1.0, 0.0)
        weight = weight + jnp.where(same, val[k : k + 1, :].astype(F32), 0.0)
    before = one_hot(iota((rows, rows), 0) < iota((rows, rows), 1))
    place_all = dot(holds.astype(BF16), before).astype(jnp.int32)
    combine = jnp.where((holds > 0.5) & (place_all == number % CAP), weight, 0.0).astype(BF16)

    in_turn(
        functools.partial(relay, GATHER_S, xs),
        functools.partial(relay, GATHER_R, xr),
    )

    loads[2].wait()
    pair_arrived(0, s1)
    for q in range(pieces):
        both = jnp.concatenate([s1[i, q * 256 : q * 256 + 256, :] for i in range(2)], axis=1)
        split = dot(apart[...], both).astype(BF16)
        s1d[q * 128 : q * 128 + 128, 0 : 2 * units] = split[:128]
        s1d[q * 128 : q * 128 + 128, 2 * units : 4 * units] = split[128:]

    gather_end(GATHER_S, xs)
    mine = dot(xs[...].reshape(total, width), s1d[...]).astype(BF16)
    part[...] = mine.reshape(n, rows, 4 * units)
    for k in far_first:
        send(SPREAD, 0, part.at[(x + k) % n], parts.at[x], x_peer(k))
    parts[x] = part[x]

    gather_end(GATHER_R, xr)
    regrouped = dot(swap[...], xr[...].reshape(total, width)).astype(BF16)
    stacked = jnp.concatenate(
        [regrouped[:, q * 128 : q * 128 + 128] for q in range(pieces)], axis=0
    )
    spread[...] = dot(stacked, expand[...]).astype(BF16).reshape(pieces, n, CAP * n, 512)

    loads[4].wait()
    pair_arrived(1, w1)
    left = jnp.concatenate(
        [
            jnp.concatenate(
                [
                    spread[q, j, :, h * 256 : h * 256 + 256]
                    for j in range(n)
                    for q in range(pieces)
                ],
                axis=1,
            )
            for h in range(2)
        ],
        axis=0,
    )
    both = dot(left, jnp.concatenate([w1[0], w1[1]], axis=1))
    gate, up = both[: CAP * n], both[CAP * n :]
    routed = (gate / (1.0 + jnp.exp(-gate)) * up).astype(BF16)

    arrived(SPREAD, 0, parts.at[pl.ds(0, n - 1)])
    pre = jnp.sum(parts[...].astype(F32), axis=0)
    gate, up = pre[:, : 2 * units], pre[:, 2 * units :]
    hidden = (gate / (1.0 + jnp.exp(-gate)) * up).astype(BF16)
    hid[...] = hidden
    for k in far_first:
        send(SHARE, 0, hid, hids.at[x], x_peer(k))
    hids[x] = hidden

    loads[5].wait()
    pair_arrived(2, w2)
    here = z * n + x
    for m in range(n):
        j = (x + m) % n
        columns = w2[:, :, pl.ds(pl.multiple_of(j * width, 128), width)]
        y[m] = dot(routed, columns.reshape(2 * units, width)).astype(BF16).reshape(n, CAP, width)
        for k in [*far_first, 0] if m else far_first:
            peer = {"expert": j, "group": at(k) * 2 + c}
            send(RETURN_R, 0, y.at[m, at(k)], placed.at[here], peer)
    placed[here] = y[0, z]

    loads[3].wait()
    pair_arrived(3, s2)
    arrived(SHARE, 0, hids.at[pl.ds(0, n - 1)])
    shared = dot(hids[...].reshape(total, 2 * units), s2[...].reshape(2 * units, width))
    ret_s[...] = shared.astype(BF16).reshape(n, rows, width)
    for k in far_first:
        send(RETURN_S, 0, ret_s.at[at(k)], got_s.at[z], z_peer(k))
    got_s[z] = ret_s[z]

    arrived(RETURN_R, 0, placed.at[pl.ds(0, n * n - 1)])
    routed_rows = lax.dot_general(
        jnp.concatenate([combine] * n, axis=0),
        placed[...].reshape(CAP * n * n, width),
        (((0,), (0,)), ((), ())),
        preferred_element_type=F32,
    )
    arrived(RETURN_S, 0, got_s.at[pl.ds(0, n - 1)])
    shared_rows = jnp.sum(got_s[...].astype(F32), axis=0)
    out_ref[...] = (routed_rows + shared_rows).astype(BF16)

    gather_sent(GATHER_S, xs)
    gather_sent(GATHER_R, xr)
    bytes_of(parts.at[pl.ds(0, n - 1)], send_sem.at[SPREAD])
    bytes_of(hids.at[pl.ds(0, n - 1)], send_sem.at[SHARE])
    bytes_of(placed.at[pl.ds(0, n * n - 1)], send_sem.at[RETURN_R])
    bytes_of(got_s.at[pl.ds(0, n - 1)], send_sem.at[RETURN_S])
    for copy in pairs:
        copy.wait_send()


def solution(mesh):
    n = mesh.shape["expert"]

    def layer(tokens, expert_ids, gate_values, gate_up, down_weight, shared_gate_up, shared_down):
        rows, features = tokens.shape
        width = features // n
        units = gate_up.shape[3]
        top = expert_ids.shape[1]
        hbm = pl.BlockSpec(memory_space=pltpu.MemorySpace.HBM)
        vmem = pl.BlockSpec(memory_space=pltpu.VMEM)
        block = pltpu.VMEM((n, rows, width), BF16)
        packed = pltpu.VMEM((n, CAP * n, width), BF16)
        return pl.pallas_call(
            functools.partial(kernel, n),
            name="moe_layer",
            out_shape=pltpu.VMEM((rows, width), BF16),
            in_specs=[hbm] * 7,
            out_specs=vmem,
            scratch_shapes=[
                block,
                pltpu.VMEM((top, rows), jnp.int32),
                pltpu.VMEM((top, rows), BF16),
                pltpu.VMEM((2, 2 * features, units), BF16),
                pltpu.VMEM((2, units, features), BF16),
                pltpu.VMEM((2, 2 * width, units), BF16),
                pltpu.VMEM((2, units, width), BF16),
                pltpu.VMEM((width, 4 * units), BF16),
                block,
                packed,
                pltpu.VMEM((n, rows, 4 * units), BF16),
                pltpu.VMEM((n, rows, 4 * units), BF16),
                pltpu.VMEM((rows, 2 * units), BF16),
                pltpu.VMEM((n, rows, 2 * units), BF16),
                pltpu.VMEM((width // 128, n, CAP * n, 512), BF16),
                pltpu.VMEM((n, n, CAP, width), BF16),
                pltpu.VMEM((n * n, CAP, width), BF16),
                block,
                block,
                pltpu.VMEM((CAP * n * n, CAP * n * n), BF16),
                pltpu.VMEM((128, 512), BF16),
                pltpu.VMEM((256, 256), BF16),
                pltpu.SemaphoreType.DMA((8,)),
                pltpu.SemaphoreType.DMA((4,)),
                pltpu.SemaphoreType.DMA((4,)),
                pltpu.SemaphoreType.DMA((SENDS,)),
                pltpu.SemaphoreType.DMA((SENDS, ARRIVALS)),
            ],
            compiler_params=pltpu.CompilerParams(
                collective_id=0, has_side_effects=True, vmem_limit_bytes=48 << 20
            ),
        )(
            *(
                pltpu.with_memory_space_constraint(a, pltpu.MemorySpace.HBM)
                for a in (
                    tokens,
                    expert_ids.T,
                    gate_values.T,
                    gate_up.reshape(2 * features, units),
                    down_weight.reshape(units, features),
                    shared_gate_up.reshape(2 * width, units),
                    shared_down,
                )
            )
        )

    return jax.shard_map(
        layer,
        mesh=mesh,
        in_specs=(
            P(("dp", "group"), None),
            P(("dp", "group"), None),
            P(("dp", "group"), None),
            P("expert", None, None, "group"),
            P("expert", "group", None),
            P("expert", None, "group"),
            P("group", "expert"),
        ),
        out_specs=P(("dp", "group"), "expert"),
        check_vma=False,
    )
```

```python
import functools

import jax
import jax.numpy as jnp
from jax import lax
from jax.experimental import pallas as pl
from jax.experimental.pallas import tpu as pltpu
from jax.sharding import PartitionSpec as P

MESH = pl.DeviceIdType.MESH
CAP = 2
F32, BF16 = jnp.float32, jnp.bfloat16
GATHER_S, GATHER_R, SPREAD, SHARE, RETURN_R, RETURN_S = range(6)
SENDS, ARRIVALS = 6, 3


def iota(shape, dim):
    return lax.broadcasted_iota(jnp.int32, shape, dim)


def one_hot(condition):
    return jnp.where(condition, 1.0, 0.0).astype(BF16)


def dot(a, b):
    return jnp.dot(a, b, preferred_element_type=F32)


def swap_matrix(n):
    rows = 2 * n * n
    to, source = iota((rows, rows), 0), iota((rows, rows), 1)
    major, minor, pick = to // (2 * n), to % (2 * n) // 2, to % 2
    return one_hot(source == minor * (2 * n) + major * 2 + pick)


def kernel(
    n,
    tok_hbm,
    ids_hbm,
    val_hbm,
    w1_hbm,
    w2_hbm,
    s1_hbm,
    s2_hbm,
    out_ref,
    tok,
    ids,
    val,
    w1,
    w2,
    s1,
    s2,
    s1d,
    xs,
    xr,
    part,
    parts,
    hid,
    hids,
    spread,
    y,
    placed,
    ret_s,
    got_s,
    swap,
    expand,
    apart,
    local_sem,
    pair_send,
    pair_recv,
    send_sem,
    recv_sem,
    ready_sem,
):
    x = lax.axis_index("expert")
    g = lax.axis_index("group")
    z, c = g // 2, g % 2
    rows, width = tok.shape[1], tok.shape[2]
    units = w2.shape[1]
    pieces = width // 128
    total = n * rows

    def z_peer(k):
        return {"group": (z + k) % n * 2 + c}

    def x_peer(k):
        return {"expert": (x + k) % n}

    sibling = {"group": z * 2 + 1 - c}

    columns = pltpu.make_async_copy(
        tok_hbm.at[:, pl.ds(pl.multiple_of(x * width, 128), width)], xs.at[z], local_sem.at[6]
    )
    columns.start()
    barrier = pltpu.get_barrier_semaphore()
    peers = [z_peer(n - 2), z_peer(n - 1), sibling]
    peers += [x_peer(k) for k in range(1, n)]

    for k in (2, 1):

        @pl.when(z < n - k)
        def _():
            pl.semaphore_signal(barrier, inc=1, device_id=z_peer(k), device_id_type=MESH)

    for peer in peers:
        pl.semaphore_signal(barrier, inc=1, device_id=peer, device_id_type=MESH)

    tokens = [
        pltpu.make_async_copy(
            tok_hbm.at[:, pl.ds(j * width, width)], tok.at[j], local_sem.at[7]
        )
        for j in range(n)
    ]
    loads = [
        pltpu.make_async_copy(source, target, local_sem.at[i])
        for i, (source, target) in enumerate(
            (
                (ids_hbm, ids),
                (val_hbm, val),
                (s1_hbm, s1.at[c]),
                (s2_hbm, s2.at[c]),
                (w1_hbm, w1.at[c]),
                (w2_hbm, w2.at[c]),
            )
        )
    ]
    for copy in [*tokens, *loads]:
        copy.start()

    def send(phase, step, source, target, peer):
        pltpu.make_async_remote_copy(
            src_ref=source,
            dst_ref=target,
            send_sem=send_sem.at[phase],
            recv_sem=recv_sem.at[phase, step],
            device_id=peer,
            device_id_type=MESH,
        ).start()

    def bytes_of(ref, sem):
        pltpu.make_async_copy(ref, ref, sem).wait()

    def arrived(phase, step, target):
        bytes_of(target, recv_sem.at[phase, step])

    upper = z >= 2
    middle = (z >= 2) & (z < n - 2)

    far_first = sorted(range(1, n), key=lambda k: (-min(k, n - k), k))
    def at(k):
        return (z + k + n) % n

    def gather_start(phase, block, steps):
        for k in steps:

            @pl.when(z >= -k)
            def _():
                own_to(phase, block, k)

    def own_to(phase, block, k):
        send(phase, {2: 0, -2: 1}.get(k, 2), block.at[z], block.at[z], z_peer(k % n))

    def gather_wrap():
        @pl.when(z == 0)
        def _():
            pl.semaphore_wait(ready_sem.at[0], 1)
            own_to(GATHER_S, xs, -2)
            own_to(GATHER_R, xr, -2)

        @pl.when(z < 2)
        def _():
            pl.semaphore_wait(ready_sem.at[1], 1)

        @pl.when(z == 0)
        def _():
            own_to(GATHER_S, xs, -1)
            own_to(GATHER_R, xr, -1)

        @pl.when(z == 1)
        def _():
            own_to(GATHER_S, xs, -2)
            own_to(GATHER_R, xr, -2)

    def relay(phase, block, sign):
        source = at(-2 * sign)
        arrived(phase, 0 if sign > 0 else 1, block.at[source])
        send(phase, 2, block.at[source], block.at[source], z_peer(sign % n))

        @pl.when(middle)
        def _():
            send(phase, 2, block.at[source], block.at[source], z_peer(2 * sign % n))

    def in_turn(*steps):
        @pl.when(upper)
        def _():
            for sign in (1, -1):
                for step in steps:
                    step(sign)

        @pl.when(jnp.logical_not(upper))
        def _():
            for sign in (-1, 1):
                for step in steps:
                    step(sign)

    def gather_end(phase, block):
        arrived(phase, 2, block.at[pl.ds(0, 5)])

    def gather_sent(phase, block):
        @pl.when(middle)
        def _():
            bytes_of(block, send_sem.at[phase])

        @pl.when(jnp.logical_not(middle))
        def _():
            bytes_of(block.at[pl.ds(0, 6)], send_sem.at[phase])

    columns.wait()
    pl.semaphore_wait(barrier, len(peers) + jnp.minimum(z, 2))

    @pl.when(z == n - 2)
    def _():
        pl.semaphore_signal(ready_sem.at[0], inc=1, device_id=z_peer(2), device_id_type=MESH)

    @pl.when(z == n - 1)
    def _():
        for k in (1, 2):
            pl.semaphore_signal(ready_sem.at[1], inc=1, device_id=z_peer(k), device_id_type=MESH)

    gather_start(GATHER_S, xs, (2, -2, 1, -1))
    pairs = [
        pltpu.make_async_remote_copy(
            src_ref=source,
            dst_ref=target.at[c],
            send_sem=pair_send.at[i],
            recv_sem=pair_recv.at[i],
            device_id=sibling,
            device_id_type=MESH,
        )
        for i, (source, target) in enumerate(
            ((s1_hbm, s1), (w1_hbm, w1), (w2_hbm, w2), (s2_hbm, s2))
        )
    ]
    pairs[0].start()

    bytes_of(tok, local_sem.at[7])
    loads[0].wait()
    named = jnp.sum(jnp.where(ids[...] == x, 1.0, 0.0), axis=0, keepdims=True)
    named = jnp.broadcast_to(named, (8, rows)).astype(BF16)
    token, lane = iota((rows, total), 0), iota((rows, total), 1)
    named_at = dot(named, one_hot(lane % rows == token))[0:1]
    place_of = dot(named, one_hot(token < lane % rows))[0:1]
    row, lane = iota((CAP * n, total), 0), iota((CAP * n, total), 1)
    picker = (named_at > 0.5) & (place_of.astype(jnp.int32) == row % CAP)
    picker = one_hot(picker & (row // CAP == lane // rows))
    packed = dot(picker, tok[...].reshape(total, width)).astype(BF16)
    xr[z] = packed
    gather_start(GATHER_R, xr, (2, -2, 1, -1))
    for copy in pairs[1:]:
        copy.start()

    def pair_arrived(i, target):
        pltpu.make_async_remote_copy(
            src_ref=target.at[1 - c],
            dst_ref=target.at[1 - c],
            send_sem=pair_send.at[i],
            recv_sem=pair_recv.at[i],
            device_id=sibling,
            device_id_type=MESH,
        ).wait_recv()

    swap[...] = swap_matrix(n)
    feature, lane = iota((128, 512), 0), iota((128, 512), 1)
    expand[...] = one_hot(lane % 256 == feature * 2 + lane // 256)
    to, source = iota((256, 256), 0), iota((256, 256), 1)
    apart[...] = one_hot(source == to % 128 * 2 + to // 128)

    loads[1].wait()
    number = iota((CAP * n, rows), 0)
    holds = jnp.zeros((CAP * n, rows), F32)
    weight = jnp.zeros((CAP * n, rows), F32)
    for k in range(ids.shape[0]):
        same = ids[k : k + 1, :] == number // CAP
        holds = holds + jnp.where(same, 1.0, 0.0)
        weight = weight + jnp.where(same, val[k : k + 1, :].astype(F32), 0.0)
    before = one_hot(iota((rows, rows), 0) < iota((rows, rows), 1))
    place_all = dot(holds.astype(BF16), before).astype(jnp.int32)
    combine = jnp.where((holds > 0.5) & (place_all == number % CAP), weight, 0.0).astype(BF16)

    gather_wrap()
    in_turn(
        functools.partial(relay, GATHER_S, xs),
        functools.partial(relay, GATHER_R, xr),
    )

    loads[2].wait()
    pair_arrived(0, s1)
    for q in range(pieces):
        both = jnp.concatenate([s1[i, q * 256 : q * 256 + 256, :] for i in range(2)], axis=1)
        split = dot(apart[...], both).astype(BF16)
        s1d[q * 128 : q * 128 + 128, 0 : 2 * units] = split[:128]
        s1d[q * 128 : q * 128 + 128, 2 * units : 4 * units] = split[128:]

    gather_end(GATHER_S, xs)
    mine = dot(xs[...].reshape(total, width), s1d[...]).astype(BF16)
    part[...] = mine.reshape(n, rows, 4 * units)
    for k in far_first:
        send(SPREAD, 0, part.at[(x + k) % n], parts.at[x], x_peer(k))
    parts[x] = part[x]

    gather_end(GATHER_R, xr)
    regrouped = dot(swap[...], xr[...].reshape(total, width)).astype(BF16)
    stacked = jnp.concatenate(
        [regrouped[:, q * 128 : q * 128 + 128] for q in range(pieces)], axis=0
    )
    spread[...] = dot(stacked, expand[...]).astype(BF16).reshape(pieces, n, CAP * n, 512)

    loads[4].wait()
    pair_arrived(1, w1)
    left = jnp.concatenate(
        [
            jnp.concatenate(
                [
                    spread[q, j, :, h * 256 : h * 256 + 256]
                    for j in range(n)
                    for q in range(pieces)
                ],
                axis=1,
            )
            for h in range(2)
        ],
        axis=0,
    )
    both = dot(left, jnp.concatenate([w1[0], w1[1]], axis=1))
    gate, up = both[: CAP * n], both[CAP * n :]
    routed = (gate / (1.0 + jnp.exp(-gate)) * up).astype(BF16)

    arrived(SPREAD, 0, parts.at[pl.ds(0, n - 1)])
    pre = jnp.sum(parts[...].astype(F32), axis=0)
    gate, up = pre[:, : 2 * units], pre[:, 2 * units :]
    hidden = (gate / (1.0 + jnp.exp(-gate)) * up).astype(BF16)
    hid[...] = hidden
    for k in far_first:
        send(SHARE, 0, hid, hids.at[x], x_peer(k))
    hids[x] = hidden

    loads[5].wait()
    pair_arrived(2, w2)
    here = z * n + x
    for m in range(n):
        j = (x + m) % n
        columns = w2[:, :, pl.ds(pl.multiple_of(j * width, 128), width)]
        y[m] = dot(routed, columns.reshape(2 * units, width)).astype(BF16).reshape(n, CAP, width)
    for t in range(n):
        for m in [*far_first, 0]:
            peer = {"expert": (x + m) % n, "group": t * 2 + c}
            if m:
                send(RETURN_R, 0, y.at[m, t], placed.at[here], peer)
            else:

                @pl.when(z != t)
                def _():
                    send(RETURN_R, 0, y.at[0, t], placed.at[here], peer)

    placed[here] = y[0, z]

    loads[3].wait()
    pair_arrived(3, s2)
    arrived(SHARE, 0, hids.at[pl.ds(0, n - 1)])
    shared = dot(hids[...].reshape(total, 2 * units), s2[...].reshape(2 * units, width))
    ret_s[...] = shared.astype(BF16).reshape(n, rows, width)
    for t in range(n):

        @pl.when(z != t)
        def _():
            send(RETURN_S, 0, ret_s.at[t], got_s.at[z], {"group": t * 2 + c})

    got_s[z] = ret_s[z]

    arrived(RETURN_R, 0, placed.at[pl.ds(0, n * n - 1)])
    routed_rows = lax.dot_general(
        jnp.concatenate([combine] * n, axis=0),
        placed[...].reshape(CAP * n * n, width),
        (((0,), (0,)), ((), ())),
        preferred_element_type=F32,
    )
    arrived(RETURN_S, 0, got_s.at[pl.ds(0, n - 1)])
    shared_rows = jnp.sum(got_s[...].astype(F32), axis=0)
    out_ref[...] = (routed_rows + shared_rows).astype(BF16)

    gather_sent(GATHER_S, xs)
    gather_sent(GATHER_R, xr)
    bytes_of(parts.at[pl.ds(0, n - 1)], send_sem.at[SPREAD])
    bytes_of(hids.at[pl.ds(0, n - 1)], send_sem.at[SHARE])
    bytes_of(placed.at[pl.ds(0, n * n - 1)], send_sem.at[RETURN_R])
    bytes_of(got_s.at[pl.ds(0, n - 1)], send_sem.at[RETURN_S])
    for copy in pairs:
        copy.wait_send()


def solution(mesh):
    n = mesh.shape["expert"]

    def layer(tokens, expert_ids, gate_values, gate_up, down_weight, shared_gate_up, shared_down):
        rows, features = tokens.shape
        width = features // n
        units = gate_up.shape[3]
        top = expert_ids.shape[1]
        hbm = pl.BlockSpec(memory_space=pltpu.MemorySpace.HBM)
        vmem = pl.BlockSpec(memory_space=pltpu.VMEM)
        block = pltpu.VMEM((n, rows, width), BF16)
        packed = pltpu.VMEM((n, CAP * n, width), BF16)
        return pl.pallas_call(
            functools.partial(kernel, n),
            name="moe_layer",
            out_shape=pltpu.VMEM((rows, width), BF16),
            in_specs=[hbm] * 7,
            out_specs=vmem,
            scratch_shapes=[
                block,
                pltpu.VMEM((top, rows), jnp.int32),
                pltpu.VMEM((top, rows), BF16),
                pltpu.VMEM((2, 2 * features, units), BF16),
                pltpu.VMEM((2, units, features), BF16),
                pltpu.VMEM((2, 2 * width, units), BF16),
                pltpu.VMEM((2, units, width), BF16),
                pltpu.VMEM((width, 4 * units), BF16),
                block,
                packed,
                pltpu.VMEM((n, rows, 4 * units), BF16),
                pltpu.VMEM((n, rows, 4 * units), BF16),
                pltpu.VMEM((rows, 2 * units), BF16),
                pltpu.VMEM((n, rows, 2 * units), BF16),
                pltpu.VMEM((width // 128, n, CAP * n, 512), BF16),
                pltpu.VMEM((n, n, CAP, width), BF16),
                pltpu.VMEM((n * n, CAP, width), BF16),
                block,
                block,
                pltpu.VMEM((CAP * n * n, CAP * n * n), BF16),
                pltpu.VMEM((128, 512), BF16),
                pltpu.VMEM((256, 256), BF16),
                pltpu.SemaphoreType.DMA((8,)),
                pltpu.SemaphoreType.DMA((4,)),
                pltpu.SemaphoreType.DMA((4,)),
                pltpu.SemaphoreType.DMA((SENDS,)),
                pltpu.SemaphoreType.DMA((SENDS, ARRIVALS)),
                pltpu.SemaphoreType.REGULAR((2,)),
            ],
            compiler_params=pltpu.CompilerParams(
                collective_id=0, has_side_effects=True, vmem_limit_bytes=48 << 20
            ),
        )(
            *(
                pltpu.with_memory_space_constraint(a, pltpu.MemorySpace.HBM)
                for a in (
                    tokens,
                    expert_ids.T,
                    gate_values.T,
                    gate_up.reshape(2 * features, units),
                    down_weight.reshape(units, features),
                    shared_gate_up.reshape(2 * width, units),
                    shared_down,
                )
            )
        )

    return jax.shard_map(
        layer,
        mesh=mesh,
        in_specs=(
            P(("dp", "group"), None),
            P(("dp", "group"), None),
            P(("dp", "group"), None),
            P("expert", None, None, "group"),
            P("expert", "group", None),
            P("expert", None, "group"),
            P("group", "expert"),
        ),
        out_specs=P(("dp", "group"), "expert"),
        check_vma=False,
    )
```

```python
import functools

import jax
import jax.numpy as jnp
from jax import lax
from jax.experimental import pallas as pl
from jax.experimental.pallas import tpu as pltpu
from jax.sharding import PartitionSpec as P

MESH = pl.DeviceIdType.MESH
CAP = 2
F32, BF16 = jnp.float32, jnp.bfloat16
GATHER_S, GATHER_R, SPREAD, SHARE, RETURN_R, RETURN_S = range(6)
SENDS, ARRIVALS = 6, 3


def iota(shape, dim):
    return lax.broadcasted_iota(jnp.int32, shape, dim)


def one_hot(condition):
    return jnp.where(condition, 1.0, 0.0).astype(BF16)


def dot(a, b):
    return jnp.dot(a, b, preferred_element_type=F32)


def swap_matrix(n):
    rows = 2 * n * n
    to, source = iota((rows, rows), 0), iota((rows, rows), 1)
    major, minor, pick = to // (2 * n), to % (2 * n) // 2, to % 2
    return one_hot(source == minor * (2 * n) + major * 2 + pick)


def kernel(
    n,
    tok_hbm,
    ids_hbm,
    val_hbm,
    w1_hbm,
    w2_hbm,
    s1_hbm,
    s2_hbm,
    out_ref,
    tok,
    ids,
    val,
    w1,
    w2,
    s1,
    s2,
    s1d,
    xs,
    xr,
    part,
    parts,
    hid,
    hids,
    spread,
    y,
    placed,
    ret_s,
    got_s,
    swap,
    expand,
    apart,
    local_sem,
    pair_send,
    pair_recv,
    send_sem,
    recv_sem,
    ready_sem,
):
    x = lax.axis_index("expert")
    g = lax.axis_index("group")
    z, c = g // 2, g % 2
    rows, width = tok.shape[1], tok.shape[2]
    units = w2.shape[1]
    pieces = width // 128
    total = n * rows

    def z_peer(k):
        return {"group": (z + k) % n * 2 + c}

    def x_peer(k):
        return {"expert": (x + k) % n}

    sibling = {"group": z * 2 + 1 - c}

    columns = pltpu.make_async_copy(
        tok_hbm.at[:, pl.ds(pl.multiple_of(x * width, 128), width)], xs.at[z], local_sem.at[6]
    )
    columns.start()
    barrier = pltpu.get_barrier_semaphore()
    peers = [z_peer(n - 2), z_peer(n - 1)]

    def rank_of(place):
        return jnp.where(place > n // 2, 2 * (n - place), jnp.maximum(2 * place - 1, 0))

    rank = rank_of(x)


    @pl.when(c == 0)
    def _():
        pl.semaphore_signal(barrier, inc=1, device_id=sibling, device_id_type=MESH)

    for k in (2, 1):

        @pl.when(z < n - k)
        def _():
            pl.semaphore_signal(barrier, inc=1, device_id=z_peer(k), device_id_type=MESH)

    for peer in peers:
        pl.semaphore_signal(barrier, inc=1, device_id=peer, device_id_type=MESH)
    for k in range(1, n):

        @pl.when(rank_of((x + k) % n) > rank)
        def _():
            pl.semaphore_signal(barrier, inc=1, device_id=x_peer(k), device_id_type=MESH)


    tokens = [
        pltpu.make_async_copy(
            tok_hbm.at[:, pl.ds(j * width, width)], tok.at[j], local_sem.at[7]
        )
        for j in range(n)
    ]
    loads = [
        pltpu.make_async_copy(source, target, local_sem.at[i])
        for i, (source, target) in enumerate(
            (
                (ids_hbm, ids),
                (val_hbm, val),
                (s1_hbm, s1.at[c]),
                (s2_hbm, s2.at[c]),
                (w1_hbm, w1.at[c]),
                (w2_hbm, w2.at[c]),
            )
        )
    ]
    for copy in [*tokens, *loads]:
        copy.start()

    def send(phase, step, source, target, peer):
        pltpu.make_async_remote_copy(
            src_ref=source,
            dst_ref=target,
            send_sem=send_sem.at[phase],
            recv_sem=recv_sem.at[phase, step],
            device_id=peer,
            device_id_type=MESH,
        ).start()

    def bytes_of(ref, sem):
        pltpu.make_async_copy(ref, ref, sem).wait()

    def arrived(phase, step, target):
        bytes_of(target, recv_sem.at[phase, step])

    upper = z >= 2
    middle = (z >= 2) & (z < n - 2)

    far_first = sorted(range(1, n), key=lambda k: (-min(k, n - k), k))
    def at(k):
        return (z + k + n) % n

    def gather_start(phase, block, steps):
        for k in steps:

            @pl.when(z >= -k)
            def _():
                own_to(phase, block, k)

    def own_to(phase, block, k):
        send(phase, {2: 0, -2: 1}.get(k, 2), block.at[z], block.at[z], z_peer(k % n))

    def gather_wrap():
        @pl.when(z == 0)
        def _():
            pl.semaphore_wait(ready_sem.at[0], 1)
            own_to(GATHER_S, xs, -2)
            own_to(GATHER_R, xr, -2)

        @pl.when(z < 2)
        def _():
            pl.semaphore_wait(ready_sem.at[1], 1)

        @pl.when(z == 0)
        def _():
            own_to(GATHER_S, xs, -1)
            own_to(GATHER_R, xr, -1)

        @pl.when(z == 1)
        def _():
            own_to(GATHER_S, xs, -2)
            own_to(GATHER_R, xr, -2)

    def relay(phase, block, sign):
        source = at(-2 * sign)
        arrived(phase, 0 if sign > 0 else 1, block.at[source])
        send(phase, 2, block.at[source], block.at[source], z_peer(sign % n))

        @pl.when(middle)
        def _():
            send(phase, 2, block.at[source], block.at[source], z_peer(2 * sign % n))

    def in_turn(*steps):
        @pl.when(upper)
        def _():
            for sign in (1, -1):
                for step in steps:
                    step(sign)

        @pl.when(jnp.logical_not(upper))
        def _():
            for sign in (-1, 1):
                for step in steps:
                    step(sign)

    def gather_end(phase, block):
        arrived(phase, 2, block.at[pl.ds(0, 5)])

    def gather_sent(phase, block):
        @pl.when(middle)
        def _():
            bytes_of(block, send_sem.at[phase])

        @pl.when(jnp.logical_not(middle))
        def _():
            bytes_of(block.at[pl.ds(0, 6)], send_sem.at[phase])

    columns.wait()
    pl.semaphore_wait(barrier, len(peers) + jnp.minimum(z, 2) + c + rank)

    @pl.when(c == 1)
    def _():
        pl.semaphore_signal(ready_sem.at[2], inc=1, device_id=sibling, device_id_type=MESH)


    @pl.when(z == n - 2)
    def _():
        pl.semaphore_signal(ready_sem.at[0], inc=1, device_id=z_peer(2), device_id_type=MESH)

    @pl.when(z == n - 1)
    def _():
        for k in (1, 2):
            pl.semaphore_signal(ready_sem.at[1], inc=1, device_id=z_peer(k), device_id_type=MESH)

    gather_start(GATHER_S, xs, (2, -2, 1, -1))
    pairs = [
        pltpu.make_async_remote_copy(
            src_ref=source,
            dst_ref=target.at[c],
            send_sem=pair_send.at[i],
            recv_sem=pair_recv.at[i],
            device_id=sibling,
            device_id_type=MESH,
        )
        for i, (source, target) in enumerate(
            ((s1_hbm, s1), (w1_hbm, w1), (w2_hbm, w2), (s2_hbm, s2))
        )
    ]

    @pl.when(c == 1)
    def _():
        pairs[0].start()


    bytes_of(tok, local_sem.at[7])
    loads[0].wait()
    named = jnp.sum(jnp.where(ids[...] == x, 1.0, 0.0), axis=0, keepdims=True)
    named = jnp.broadcast_to(named, (8, rows)).astype(BF16)
    token, lane = iota((rows, total), 0), iota((rows, total), 1)
    named_at = dot(named, one_hot(lane % rows == token))[0:1]
    place_of = dot(named, one_hot(token < lane % rows))[0:1]
    row, lane = iota((CAP * n, total), 0), iota((CAP * n, total), 1)
    picker = (named_at > 0.5) & (place_of.astype(jnp.int32) == row % CAP)
    picker = one_hot(picker & (row // CAP == lane // rows))
    packed = dot(picker, tok[...].reshape(total, width)).astype(BF16)
    xr[z] = packed
    gather_start(GATHER_R, xr, (2, -2, 1, -1))

    @pl.when(c == 1)
    def _():
        for copy in pairs[1:]:
            copy.start()


    def pair_arrived(i, target):
        pltpu.make_async_remote_copy(
            src_ref=target.at[1 - c],
            dst_ref=target.at[1 - c],
            send_sem=pair_send.at[i],
            recv_sem=pair_recv.at[i],
            device_id=sibling,
            device_id_type=MESH,
        ).wait_recv()

    swap[...] = swap_matrix(n)
    feature, lane = iota((128, 512), 0), iota((128, 512), 1)
    expand[...] = one_hot(lane % 256 == feature * 2 + lane // 256)
    to, source = iota((256, 256), 0), iota((256, 256), 1)
    apart[...] = one_hot(source == to % 128 * 2 + to // 128)

    for k in range(1, n):

        @pl.when(rank_of((x + k) % n) < rank)
        def _():
            pl.semaphore_signal(
                ready_sem.at[3], inc=1, device_id=x_peer(k), device_id_type=MESH
            )

    loads[1].wait()
    number = iota((CAP * n, rows), 0)
    holds = jnp.zeros((CAP * n, rows), F32)
    weight = jnp.zeros((CAP * n, rows), F32)
    for k in range(ids.shape[0]):
        same = ids[k : k + 1, :] == number // CAP
        holds = holds + jnp.where(same, 1.0, 0.0)
        weight = weight + jnp.where(same, val[k : k + 1, :].astype(F32), 0.0)
    before = one_hot(iota((rows, rows), 0) < iota((rows, rows), 1))
    place_all = dot(holds.astype(BF16), before).astype(jnp.int32)
    combine = jnp.where((holds > 0.5) & (place_all == number % CAP), weight, 0.0).astype(BF16)

    @pl.when(c == 0)
    def _():
        pl.semaphore_wait(ready_sem.at[2], 1)
        for copy in pairs:
            copy.start()

    gather_wrap()
    in_turn(
        functools.partial(relay, GATHER_S, xs),
        functools.partial(relay, GATHER_R, xr),
    )

    loads[2].wait()
    pair_arrived(0, s1)
    for q in range(pieces):
        both = jnp.concatenate([s1[i, q * 256 : q * 256 + 256, :] for i in range(2)], axis=1)
        split = dot(apart[...], both).astype(BF16)
        s1d[q * 128 : q * 128 + 128, 0 : 2 * units] = split[:128]
        s1d[q * 128 : q * 128 + 128, 2 * units : 4 * units] = split[128:]

    gather_end(GATHER_S, xs)
    @pl.when(rank < n - 1)
    def _():
        pl.semaphore_wait(ready_sem.at[3], n - 1 - rank)

    mine = dot(xs[...].reshape(total, width), s1d[...]).astype(BF16)
    part[...] = mine.reshape(n, rows, 4 * units)
    for k in far_first:
        send(SPREAD, 0, part.at[(x + k) % n], parts.at[x], x_peer(k))
    parts[x] = part[x]

    gather_end(GATHER_R, xr)
    regrouped = dot(swap[...], xr[...].reshape(total, width)).astype(BF16)
    stacked = jnp.concatenate(
        [regrouped[:, q * 128 : q * 128 + 128] for q in range(pieces)], axis=0
    )
    spread[...] = dot(stacked, expand[...]).astype(BF16).reshape(pieces, n, CAP * n, 512)

    loads[4].wait()
    pair_arrived(1, w1)
    left = jnp.concatenate(
        [
            jnp.concatenate(
                [
                    spread[q, j, :, h * 256 : h * 256 + 256]
                    for j in range(n)
                    for q in range(pieces)
                ],
                axis=1,
            )
            for h in range(2)
        ],
        axis=0,
    )
    both = dot(left, jnp.concatenate([w1[0], w1[1]], axis=1))
    gate, up = both[: CAP * n], both[CAP * n :]
    routed = (gate / (1.0 + jnp.exp(-gate)) * up).astype(BF16)

    arrived(SPREAD, 0, parts.at[pl.ds(0, n - 1)])
    pre = jnp.sum(parts[...].astype(F32), axis=0)
    gate, up = pre[:, : 2 * units], pre[:, 2 * units :]
    hidden = (gate / (1.0 + jnp.exp(-gate)) * up).astype(BF16)
    hid[...] = hidden
    for k in far_first:
        send(SHARE, 0, hid, hids.at[x], x_peer(k))
    hids[x] = hidden

    loads[5].wait()
    pair_arrived(2, w2)
    here = z * n + x
    for m in range(n):
        j = (x + m) % n
        columns = w2[:, :, pl.ds(pl.multiple_of(j * width, 128), width)]
        y[m] = dot(routed, columns.reshape(2 * units, width)).astype(BF16).reshape(n, CAP, width)
    for t in range(n):
        for m in [*far_first, 0]:
            peer = {"expert": (x + m) % n, "group": t * 2 + c}
            if m:
                send(RETURN_R, 0, y.at[m, t], placed.at[here], peer)
            else:

                @pl.when(z != t)
                def _():
                    send(RETURN_R, 0, y.at[0, t], placed.at[here], peer)

    placed[here] = y[0, z]

    loads[3].wait()
    pair_arrived(3, s2)
    arrived(SHARE, 0, hids.at[pl.ds(0, n - 1)])
    shared = dot(hids[...].reshape(total, 2 * units), s2[...].reshape(2 * units, width))
    ret_s[...] = shared.astype(BF16).reshape(n, rows, width)
    for t in range(n):

        @pl.when(z != t)
        def _():
            send(RETURN_S, 0, ret_s.at[t], got_s.at[z], {"group": t * 2 + c})

    got_s[z] = ret_s[z]

    arrived(RETURN_R, 0, placed.at[pl.ds(0, n * n - 1)])
    routed_rows = lax.dot_general(
        jnp.concatenate([combine] * n, axis=0),
        placed[...].reshape(CAP * n * n, width),
        (((0,), (0,)), ((), ())),
        preferred_element_type=F32,
    )
    arrived(RETURN_S, 0, got_s.at[pl.ds(0, n - 1)])
    shared_rows = jnp.sum(got_s[...].astype(F32), axis=0)
    out_ref[...] = (routed_rows + shared_rows).astype(BF16)

    gather_sent(GATHER_S, xs)
    gather_sent(GATHER_R, xr)
    bytes_of(parts.at[pl.ds(0, n - 1)], send_sem.at[SPREAD])
    bytes_of(hids.at[pl.ds(0, n - 1)], send_sem.at[SHARE])
    bytes_of(placed.at[pl.ds(0, n * n - 1)], send_sem.at[RETURN_R])
    bytes_of(got_s.at[pl.ds(0, n - 1)], send_sem.at[RETURN_S])
    for copy in pairs:
        copy.wait_send()


def solution(mesh):
    n = mesh.shape["expert"]

    def layer(tokens, expert_ids, gate_values, gate_up, down_weight, shared_gate_up, shared_down):
        rows, features = tokens.shape
        width = features // n
        units = gate_up.shape[3]
        top = expert_ids.shape[1]
        hbm = pl.BlockSpec(memory_space=pltpu.MemorySpace.HBM)
        vmem = pl.BlockSpec(memory_space=pltpu.VMEM)
        block = pltpu.VMEM((n, rows, width), BF16)
        packed = pltpu.VMEM((n, CAP * n, width), BF16)
        return pl.pallas_call(
            functools.partial(kernel, n),
            name="moe_layer",
            out_shape=pltpu.VMEM((rows, width), BF16),
            in_specs=[hbm] * 7,
            out_specs=vmem,
            scratch_shapes=[
                block,
                pltpu.VMEM((top, rows), jnp.int32),
                pltpu.VMEM((top, rows), BF16),
                pltpu.VMEM((2, 2 * features, units), BF16),
                pltpu.VMEM((2, units, features), BF16),
                pltpu.VMEM((2, 2 * width, units), BF16),
                pltpu.VMEM((2, units, width), BF16),
                pltpu.VMEM((width, 4 * units), BF16),
                block,
                packed,
                pltpu.VMEM((n, rows, 4 * units), BF16),
                pltpu.VMEM((n, rows, 4 * units), BF16),
                pltpu.VMEM((rows, 2 * units), BF16),
                pltpu.VMEM((n, rows, 2 * units), BF16),
                pltpu.VMEM((width // 128, n, CAP * n, 512), BF16),
                pltpu.VMEM((n, n, CAP, width), BF16),
                pltpu.VMEM((n * n, CAP, width), BF16),
                block,
                block,
                pltpu.VMEM((CAP * n * n, CAP * n * n), BF16),
                pltpu.VMEM((128, 512), BF16),
                pltpu.VMEM((256, 256), BF16),
                pltpu.SemaphoreType.DMA((8,)),
                pltpu.SemaphoreType.DMA((4,)),
                pltpu.SemaphoreType.DMA((4,)),
                pltpu.SemaphoreType.DMA((SENDS,)),
                pltpu.SemaphoreType.DMA((SENDS, ARRIVALS)),
                pltpu.SemaphoreType.REGULAR((4,)),
            ],
            compiler_params=pltpu.CompilerParams(
                collective_id=0, has_side_effects=True, vmem_limit_bytes=48 << 20
            ),
        )(
            *(
                pltpu.with_memory_space_constraint(a, pltpu.MemorySpace.HBM)
                for a in (
                    tokens,
                    expert_ids.T,
                    gate_values.T,
                    gate_up.reshape(2 * features, units),
                    down_weight.reshape(units, features),
                    shared_gate_up.reshape(2 * width, units),
                    shared_down,
                )
            )
        )

    return jax.shard_map(
        layer,
        mesh=mesh,
        in_specs=(
            P(("dp", "group"), None),
            P(("dp", "group"), None),
            P(("dp", "group"), None),
            P("expert", None, None, "group"),
            P("expert", "group", None),
            P("expert", None, "group"),
            P("group", "expert"),
        ),
        out_specs=P(("dp", "group"), "expert"),
        check_vma=False,
    )
```

```python
import functools

import jax
import jax.numpy as jnp
from jax import lax
from jax.experimental import pallas as pl
from jax.experimental.pallas import tpu as pltpu
from jax.sharding import PartitionSpec as P

MESH = pl.DeviceIdType.MESH
CAP = 2
F32, BF16 = jnp.float32, jnp.bfloat16
GATHER_S, GATHER_R, SPREAD, SHARE, RETURN_R, RETURN_S = range(6)
SENDS, ARRIVALS = 6, 3


def iota(shape, dim):
    return lax.broadcasted_iota(jnp.int32, shape, dim)


def one_hot(condition):
    return jnp.where(condition, 1.0, 0.0).astype(BF16)


def dot(a, b):
    return jnp.dot(a, b, preferred_element_type=F32)


def swap_matrix(n):
    rows = 2 * n * n
    to, source = iota((rows, rows), 0), iota((rows, rows), 1)
    major, minor, pick = to // (2 * n), to % (2 * n) // 2, to % 2
    return one_hot(source == minor * (2 * n) + major * 2 + pick)


def kernel(
    n,
    tok_hbm,
    ids_hbm,
    val_hbm,
    w1_hbm,
    w2_hbm,
    s1_hbm,
    s2_hbm,
    out_ref,
    tok,
    ids,
    val,
    w1,
    w2,
    s1,
    s2,
    s1d,
    xs,
    xr,
    part,
    parts,
    hid,
    hids,
    spread,
    y,
    placed,
    ret_s,
    got_s,
    swap,
    expand,
    apart,
    local_sem,
    pair_send,
    pair_recv,
    send_sem,
    recv_sem,
    ready_sem,
):
    x = lax.axis_index("expert")
    g = lax.axis_index("group")
    z, c = g // 2, g % 2
    rows, width = tok.shape[1], tok.shape[2]
    units = w2.shape[1]
    pieces = width // 128
    total = n * rows

    def z_peer(k):
        return {"group": (z + k) % n * 2 + c}

    def x_peer(k):
        return {"expert": (x + k) % n}

    sibling = {"group": z * 2 + 1 - c}

    columns = pltpu.make_async_copy(
        tok_hbm.at[:, pl.ds(pl.multiple_of(x * width, 128), width)], xs.at[z], local_sem.at[6]
    )
    columns.start()
    barrier = pltpu.get_barrier_semaphore()
    peers = [z_peer(n - 2), z_peer(n - 1)]

    def rank_of(place):
        return jnp.where(place > n // 2, 2 * (n - place), jnp.maximum(2 * place - 1, 0))

    rank = rank_of(x)


    @pl.when(c == 0)
    def _():
        pl.semaphore_signal(barrier, inc=1, device_id=sibling, device_id_type=MESH)

    for k in (2, 1):

        @pl.when(z < n - k)
        def _():
            pl.semaphore_signal(barrier, inc=1, device_id=z_peer(k), device_id_type=MESH)

    for peer in peers:
        pl.semaphore_signal(barrier, inc=1, device_id=peer, device_id_type=MESH)
    for k in range(1, n):

        @pl.when(rank_of((x + k) % n) > rank)
        def _():
            pl.semaphore_signal(barrier, inc=1, device_id=x_peer(k), device_id_type=MESH)


    tokens = [
        pltpu.make_async_copy(
            tok_hbm.at[:, pl.ds(j * width, width)], tok.at[j], local_sem.at[7]
        )
        for j in range(n)
    ]
    loads = [
        pltpu.make_async_copy(source, target, local_sem.at[i])
        for i, (source, target) in enumerate(
            (
                (ids_hbm, ids),
                (val_hbm, val),
                (s1_hbm, s1.at[c]),
                (s2_hbm, s2.at[c]),
                (w1_hbm, w1.at[c]),
                (w2_hbm, w2.at[c]),
            )
        )
    ]
    for copy in [*tokens, *loads]:
        copy.start()

    def send(phase, step, source, target, peer):
        pltpu.make_async_remote_copy(
            src_ref=source,
            dst_ref=target,
            send_sem=send_sem.at[phase],
            recv_sem=recv_sem.at[phase, step],
            device_id=peer,
            device_id_type=MESH,
        ).start()

    def bytes_of(ref, sem):
        pltpu.make_async_copy(ref, ref, sem).wait()

    def arrived(phase, step, target):
        bytes_of(target, recv_sem.at[phase, step])

    upper = z >= 2
    middle = (z >= 2) & (z < n - 2)

    far_first = sorted(range(1, n), key=lambda k: (-min(k, n - k), k))
    def at(k):
        return (z + k + n) % n

    def gather_start(phase, block, steps):
        for k in steps:

            @pl.when(z >= -k)
            def _():
                own_to(phase, block, k)

    def own_to(phase, block, k):
        send(phase, {2: 0, -2: 1}.get(k, 2), block.at[z], block.at[z], z_peer(k % n))

    def gather_wrap():
        @pl.when(z == 0)
        def _():
            pl.semaphore_wait(ready_sem.at[0], 1)
            own_to(GATHER_S, xs, -2)
            own_to(GATHER_R, xr, -2)

        @pl.when(z < 2)
        def _():
            pl.semaphore_wait(ready_sem.at[1], 1)

        @pl.when(z == 0)
        def _():
            own_to(GATHER_S, xs, -1)
            own_to(GATHER_R, xr, -1)

        @pl.when(z == 1)
        def _():
            own_to(GATHER_S, xs, -2)
            own_to(GATHER_R, xr, -2)

    def relay(phase, block, sign):
        source = at(-2 * sign)
        arrived(phase, 0 if sign > 0 else 1, block.at[source])
        send(phase, 2, block.at[source], block.at[source], z_peer(sign % n))

        @pl.when(middle)
        def _():
            send(phase, 2, block.at[source], block.at[source], z_peer(2 * sign % n))

    def in_turn(*steps):
        @pl.when(upper)
        def _():
            for sign in (1, -1):
                for step in steps:
                    step(sign)

        @pl.when(jnp.logical_not(upper))
        def _():
            for sign in (-1, 1):
                for step in steps:
                    step(sign)

    def gather_end(phase, block):
        arrived(phase, 2, block.at[pl.ds(0, 5)])

    def gather_sent(phase, block):
        @pl.when(middle)
        def _():
            bytes_of(block, send_sem.at[phase])

        @pl.when(jnp.logical_not(middle))
        def _():
            bytes_of(block.at[pl.ds(0, 6)], send_sem.at[phase])

    columns.wait()
    pl.semaphore_wait(barrier, len(peers) + jnp.minimum(z, 2) + c + rank)

    @pl.when(c == 1)
    def _():
        pl.semaphore_signal(ready_sem.at[2], inc=1, device_id=sibling, device_id_type=MESH)


    @pl.when(z == n - 2)
    def _():
        pl.semaphore_signal(ready_sem.at[0], inc=1, device_id=z_peer(2), device_id_type=MESH)

    @pl.when(z == n - 1)
    def _():
        for k in (1, 2):
            pl.semaphore_signal(ready_sem.at[1], inc=1, device_id=z_peer(k), device_id_type=MESH)

    gather_start(GATHER_S, xs, (2, -2, 1, -1))
    pairs = [
        pltpu.make_async_remote_copy(
            src_ref=source,
            dst_ref=target.at[c],
            send_sem=pair_send.at[i],
            recv_sem=pair_recv.at[i],
            device_id=sibling,
            device_id_type=MESH,
        )
        for i, (source, target) in enumerate(
            ((s1_hbm, s1), (w1_hbm, w1), (w2_hbm, w2), (s2_hbm, s2))
        )
    ]

    @pl.when(c == 1)
    def _():
        pairs[0].start()


    bytes_of(tok, local_sem.at[7])
    loads[0].wait()
    named = jnp.sum(jnp.where(ids[...] == x, 1.0, 0.0), axis=0, keepdims=True)
    named = jnp.broadcast_to(named, (8, rows)).astype(BF16)
    token, lane = iota((rows, total), 0), iota((rows, total), 1)
    named_at = dot(named, one_hot(lane % rows == token))[0:1]
    place_of = dot(named, one_hot(token < lane % rows))[0:1]
    row, lane = iota((CAP * n, total), 0), iota((CAP * n, total), 1)
    picker = (named_at > 0.5) & (place_of.astype(jnp.int32) == row % CAP)
    picker = one_hot(picker & (row // CAP == lane // rows))
    packed = dot(picker, tok[...].reshape(total, width)).astype(BF16)
    xr[z] = packed
    gather_start(GATHER_R, xr, (2, -2, 1, -1))

    @pl.when(c == 1)
    def _():
        for copy in pairs[1:]:
            copy.start()


    def pair_arrived(i, target):
        pltpu.make_async_remote_copy(
            src_ref=target.at[1 - c],
            dst_ref=target.at[1 - c],
            send_sem=pair_send.at[i],
            recv_sem=pair_recv.at[i],
            device_id=sibling,
            device_id_type=MESH,
        ).wait_recv()

    swap[...] = swap_matrix(n)
    feature, lane = iota((128, 512), 0), iota((128, 512), 1)
    expand[...] = one_hot(lane % 256 == feature * 2 + lane // 256)
    to, source = iota((256, 256), 0), iota((256, 256), 1)
    apart[...] = one_hot(source == to % 128 * 2 + to // 128)

    for k in range(1, n):

        @pl.when(rank_of((x + k) % n) < rank)
        def _():
            pl.semaphore_signal(
                ready_sem.at[3], inc=1, device_id=x_peer(k), device_id_type=MESH
            )

    loads[1].wait()
    number = iota((CAP * n, rows), 0)
    holds = jnp.zeros((CAP * n, rows), F32)
    weight = jnp.zeros((CAP * n, rows), F32)
    for k in range(ids.shape[0]):
        same = ids[k : k + 1, :] == number // CAP
        holds = holds + jnp.where(same, 1.0, 0.0)
        weight = weight + jnp.where(same, val[k : k + 1, :].astype(F32), 0.0)
    before = one_hot(iota((rows, rows), 0) < iota((rows, rows), 1))
    place_all = dot(holds.astype(BF16), before).astype(jnp.int32)
    combine = jnp.where((holds > 0.5) & (place_all == number % CAP), weight, 0.0).astype(BF16)

    @pl.when(c == 0)
    def _():
        pl.semaphore_wait(ready_sem.at[2], 1)
        for copy in pairs:
            copy.start()

    gather_wrap()
    in_turn(
        functools.partial(relay, GATHER_S, xs),
        functools.partial(relay, GATHER_R, xr),
    )

    loads[2].wait()
    pair_arrived(0, s1)
    for q in range(pieces):
        both = jnp.concatenate([s1[i, q * 256 : q * 256 + 256, :] for i in range(2)], axis=1)
        split = dot(apart[...], both).astype(BF16)
        s1d[q * 128 : q * 128 + 128, 0 : 2 * units] = split[:128]
        s1d[q * 128 : q * 128 + 128, 2 * units : 4 * units] = split[128:]

    gather_end(GATHER_S, xs)
    @pl.when(rank < n - 1)
    def _():
        pl.semaphore_wait(ready_sem.at[3], n - 1 - rank)

    mine = dot(xs[...].reshape(total, width), s1d[...]).astype(BF16)
    part[...] = mine.reshape(n, rows, 4 * units)
    for k in far_first:
        send(SPREAD, 0, part.at[(x + k) % n], parts.at[x], x_peer(k))
    parts[x] = part[x]

    gather_end(GATHER_R, xr)
    regrouped = dot(swap[...], xr[...].reshape(total, width)).astype(BF16)
    stacked = jnp.concatenate(
        [regrouped[:, q * 128 : q * 128 + 128] for q in range(pieces)], axis=0
    )
    spread[...] = dot(stacked, expand[...]).astype(BF16).reshape(pieces, n, CAP * n, 512)

    def share():
        arrived(SPREAD, 0, parts.at[pl.ds(0, n - 1)])
        pre = jnp.sum(parts[...].astype(F32), axis=0)
        gate, up = pre[:, : 2 * units], pre[:, 2 * units :]
        hidden = (gate / (1.0 + jnp.exp(-gate)) * up).astype(BF16)
        hid[...] = hidden
        for k in far_first:
            send(SHARE, 0, hid, hids.at[x], x_peer(k))
        hids[x] = hidden

    @pl.when(c == 1)
    def _():
        share()

    loads[4].wait()
    pair_arrived(1, w1)
    left = jnp.concatenate(
        [
            jnp.concatenate(
                [
                    spread[q, j, :, h * 256 : h * 256 + 256]
                    for j in range(n)
                    for q in range(pieces)
                ],
                axis=1,
            )
            for h in range(2)
        ],
        axis=0,
    )
    both = dot(left, jnp.concatenate([w1[0], w1[1]], axis=1))
    gate, up = both[: CAP * n], both[CAP * n :]
    routed = (gate / (1.0 + jnp.exp(-gate)) * up).astype(BF16)

    @pl.when(c == 0)
    def _():
        share()

    loads[5].wait()
    pair_arrived(2, w2)
    here = z * n + x
    for m in range(n):
        j = (x + m) % n
        columns = w2[:, :, pl.ds(pl.multiple_of(j * width, 128), width)]
        y[m] = dot(routed, columns.reshape(2 * units, width)).astype(BF16).reshape(n, CAP, width)
    for t in range(n):
        for m in [*far_first, 0]:
            peer = {"expert": (x + m) % n, "group": t * 2 + c}
            if m:
                send(RETURN_R, 0, y.at[m, t], placed.at[here], peer)
            else:

                @pl.when(z != t)
                def _():
                    send(RETURN_R, 0, y.at[0, t], placed.at[here], peer)

    placed[here] = y[0, z]

    loads[3].wait()
    pair_arrived(3, s2)
    arrived(SHARE, 0, hids.at[pl.ds(0, n - 1)])
    shared = dot(hids[...].reshape(total, 2 * units), s2[...].reshape(2 * units, width))
    ret_s[...] = shared.astype(BF16).reshape(n, rows, width)
    for t in range(n):

        @pl.when(z != t)
        def _():
            send(RETURN_S, 0, ret_s.at[t], got_s.at[z], {"group": t * 2 + c})

    got_s[z] = ret_s[z]

    arrived(RETURN_R, 0, placed.at[pl.ds(0, n * n - 1)])
    routed_rows = lax.dot_general(
        jnp.concatenate([combine] * n, axis=0),
        placed[...].reshape(CAP * n * n, width),
        (((0,), (0,)), ((), ())),
        preferred_element_type=F32,
    )
    arrived(RETURN_S, 0, got_s.at[pl.ds(0, n - 1)])
    shared_rows = jnp.sum(got_s[...].astype(F32), axis=0)
    out_ref[...] = (routed_rows + shared_rows).astype(BF16)

    gather_sent(GATHER_S, xs)
    gather_sent(GATHER_R, xr)
    bytes_of(parts.at[pl.ds(0, n - 1)], send_sem.at[SPREAD])
    bytes_of(hids.at[pl.ds(0, n - 1)], send_sem.at[SHARE])
    bytes_of(placed.at[pl.ds(0, n * n - 1)], send_sem.at[RETURN_R])
    bytes_of(got_s.at[pl.ds(0, n - 1)], send_sem.at[RETURN_S])
    for copy in pairs:
        copy.wait_send()


def solution(mesh):
    n = mesh.shape["expert"]

    def layer(tokens, expert_ids, gate_values, gate_up, down_weight, shared_gate_up, shared_down):
        rows, features = tokens.shape
        width = features // n
        units = gate_up.shape[3]
        top = expert_ids.shape[1]
        hbm = pl.BlockSpec(memory_space=pltpu.MemorySpace.HBM)
        vmem = pl.BlockSpec(memory_space=pltpu.VMEM)
        block = pltpu.VMEM((n, rows, width), BF16)
        packed = pltpu.VMEM((n, CAP * n, width), BF16)
        return pl.pallas_call(
            functools.partial(kernel, n),
            name="moe_layer",
            out_shape=pltpu.VMEM((rows, width), BF16),
            in_specs=[hbm] * 7,
            out_specs=vmem,
            scratch_shapes=[
                block,
                pltpu.VMEM((top, rows), jnp.int32),
                pltpu.VMEM((top, rows), BF16),
                pltpu.VMEM((2, 2 * features, units), BF16),
                pltpu.VMEM((2, units, features), BF16),
                pltpu.VMEM((2, 2 * width, units), BF16),
                pltpu.VMEM((2, units, width), BF16),
                pltpu.VMEM((width, 4 * units), BF16),
                block,
                packed,
                pltpu.VMEM((n, rows, 4 * units), BF16),
                pltpu.VMEM((n, rows, 4 * units), BF16),
                pltpu.VMEM((rows, 2 * units), BF16),
                pltpu.VMEM((n, rows, 2 * units), BF16),
                pltpu.VMEM((width // 128, n, CAP * n, 512), BF16),
                pltpu.VMEM((n, n, CAP, width), BF16),
                pltpu.VMEM((n * n, CAP, width), BF16),
                block,
                block,
                pltpu.VMEM((CAP * n * n, CAP * n * n), BF16),
                pltpu.VMEM((128, 512), BF16),
                pltpu.VMEM((256, 256), BF16),
                pltpu.SemaphoreType.DMA((8,)),
                pltpu.SemaphoreType.DMA((4,)),
                pltpu.SemaphoreType.DMA((4,)),
                pltpu.SemaphoreType.DMA((SENDS,)),
                pltpu.SemaphoreType.DMA((SENDS, ARRIVALS)),
                pltpu.SemaphoreType.REGULAR((4,)),
            ],
            compiler_params=pltpu.CompilerParams(
                collective_id=0, has_side_effects=True, vmem_limit_bytes=48 << 20
            ),
        )(
            *(
                pltpu.with_memory_space_constraint(a, pltpu.MemorySpace.HBM)
                for a in (
                    tokens,
                    expert_ids.T,
                    gate_values.T,
                    gate_up.reshape(2 * features, units),
                    down_weight.reshape(units, features),
                    shared_gate_up.reshape(2 * width, units),
                    shared_down,
                )
            )
        )

    return jax.shard_map(
        layer,
        mesh=mesh,
        in_specs=(
            P(("dp", "group"), None),
            P(("dp", "group"), None),
            P(("dp", "group"), None),
            P("expert", None, None, "group"),
            P("expert", "group", None),
            P("expert", None, "group"),
            P("group", "expert"),
        ),
        out_specs=P(("dp", "group"), "expert"),
        check_vma=False,
    )
```
